32 devices in a mesh: dp: 2 (over x), fsdp: 4 (over z), mp: 4 (over y, core).
Axes of the slice: x: 2, y: 2, z: 4, core: 2. Of those that a mesh axis runs over, the one named last changes fastest.
Arguments:
- gradients: bfloat16 [8, 12, 2, 256, 1024], P(('dp', 'fsdp'), None, None, None, 'mp'), may hold values from -6 to 6
- master: float32 [12, 2, 256, 1024], P(None, None, ('dp', 'fsdp'), 'mp'), may hold values from -0.375 to 0.375
- teacher: float32 [12, 2, 256, 1024], P(None, None, ('dp', 'fsdp'), 'mp'), may hold values from -0.375 to 0.375
- first_moment: float32 [12, 2, 256, 1024], P(None, None, ('dp', 'fsdp'), 'mp'), may hold values from -2.2888184e-05 to 2.2888184e-05
- second_moment: float32 [12, 2, 256, 1024], P(None, None, ('dp', 'fsdp'), 'mp'), may hold values from 0 to 1, as said below
- layer_rates: float32 [12], replicated, may hold values from 0.02 to 0.2
Outputs:
- master_new: float32 [12, 2, 256, 1024], P(None, None, ('dp', 'fsdp'), 'mp')
- teacher_new: float32 [12, 2, 256, 1024], P(None, None, ('dp', 'fsdp'), 'mp')
- first_new: float32 [12, 2, 256, 1024], P(None, None, ('dp', 'fsdp'), 'mp')
- second_new: float32 [12, 2, 256, 1024], P(None, None, ('dp', 'fsdp'), 'mp')
- student_weights: bfloat16 [12, 2, 256, 1024], P(None, None, None, 'mp')
- teacher_weights: bfloat16 [12, 2, 256, 1024], P(None, None, None, 'mp')
The draws below stay inside these ranges and needn't reach their ends.
Inputs may be any that keep to these rules, and one draw needn't show every extreme that they name: `second_moment`: every entry is positive.
All inputs are finite; a program needn't handle non-finite values.
Results may differ from the reference program's by a relative error of at most 0.0004.
Values may be sent and summed in bfloat16 or wider, within the bound.
A program may use at most 64 MiB of HBM per device.

```python
import math
import jax
import jax.numpy as jnp
from jax import lax

D = 256
FF = 1024
LAYERS = 12
NDATA = 8


def draw_second_moment(key, part):
    typical = 0.01 / (2.0 * LAYERS * D * FF)
    spread = jax.random.uniform(key, (LAYERS, 2, D, FF), jnp.float32, -2.3, 2.3)
    return typical * jnp.exp(spread)


def spiked(entries, rng, source, target, blocks, factor):
    def block_of(axis_at):
        return (jnp.arange(entries.shape[axis_at]) // (entries.shape[axis_at] // blocks)).reshape((-1,) + (1,) * (entries.ndim - 1 - axis_at))

    first = jax.random.permutation(rng, blocks)[block_of(target)]
    other_side = (block_of(target) + blocks // 2) % blocks
    return jnp.where((block_of(source) == first) | (block_of(source) == other_side), factor * entries, entries)


def level_of(rng, extent, pieces, low, largest):
    factor_of, own = 1.0, jax.random.fold_in(rng, 6)
    for dim, parts in pieces:
        heights = jnp.exp(jax.random.uniform(jax.random.fold_in(own, dim), (parts,), jnp.float32, low / len(pieces), largest / len(pieces)))
        factor_of = factor_of * jnp.repeat(heights, extent[dim] // parts).reshape([-1 if axis == dim else 1 for axis in range(len(extent))])
    return factor_of


def noise(key, extent, width, reach, pieces=(), held_as=jnp.bfloat16):
    drawn = width * jax.random.normal(key, extent, jnp.float32)
    if pieces:
        drawn = drawn * level_of(key, extent, pieces, -0.22, 0.18)
    return jnp.clip(drawn, -reach, reach).astype(held_as)


def gaussian_with(own_key, shape, deviation, reach, split, heavy, dtype=jnp.bfloat16):
    drawn = deviation * jax.random.normal(own_key, shape, jnp.float32)
    if split:
        drawn = drawn * level_of(own_key, shape, split, -0.22, 0.18)
    return jnp.clip(spiked(drawn, jax.random.fold_in(own_key, 3), *heavy), -reach, reach).astype(dtype)


def setup_inputs(seed: int = 0) -> dict:
    keys = jax.random.split(jax.random.key(seed), 7)
    gradients = gaussian_with(keys[0], (NDATA, LAYERS, 2, D, FF), 1.0, 6.0, ((0, 8), (4, 4)), (0, 3, 8, 2.0))
    master = noise(keys[1], (LAYERS, 2, D, FF), D ** -0.5, 0.375, ((2, 8), (3, 4)), jnp.float32)
    teacher = noise(keys[2], (LAYERS, 2, D, FF), D ** -0.5, 0.375, ((2, 8), (3, 4)), jnp.float32)
    first_moment = noise(keys[3], (LAYERS, 2, D, FF), (20000 * LAYERS * D * FF) ** -0.5, 2.288818359375e-05, ((2, 8), (3, 4)), jnp.float32)
    second_moment = draw_second_moment(jax.random.fold_in(keys[6], 71), 0)
    layer_rates = jnp.clip(jnp.exp(jax.random.uniform(keys[5], (LAYERS,), jnp.float32, math.log(0.02), math.log(0.2))), 0.02, 0.2)
    return {"gradients": gradients, "master": master, "teacher": teacher, "first_moment": first_moment, "second_moment": second_moment, "layer_rates": layer_rates}


CLIP_NORM = 0.1
BETA_ONE = 0.9
BETA_TWO = 0.999
BIAS_ONE = 1.0 - 0.9 ** 50 * 0.9 ** 50
BIAS_TWO = 1.0 - 0.999 ** 50 * 0.999 ** 50
ADAM_EPS = 1e-08
DECAY = 0.05
EMA_KEEP = 0.95

def accumulate(carry, piece):
    return (carry + piece.astype(jnp.float32), jnp.zeros((), jnp.float32))

def reference(gradients, master, teacher, first_moment, second_moment, layer_rates):
    summed, unused = lax.scan(accumulate, jnp.zeros(gradients.shape[1:], jnp.float32), gradients)
    mean_grad = summed / gradients.shape[0]
    norm_sq = jnp.sum(mean_grad * mean_grad)
    clip_factor = jnp.minimum(1.0, CLIP_NORM / (jnp.sqrt(norm_sq) + 1e-06))
    clipped = clip_factor * mean_grad
    first_new = BETA_ONE * first_moment + (1.0 - BETA_ONE) * clipped
    second_new = BETA_TWO * second_moment + (1.0 - BETA_TWO) * clipped * clipped
    direction = first_new / BIAS_ONE / (jnp.sqrt(second_new / BIAS_TWO) + ADAM_EPS) + DECAY * master
    layer_rate = layer_rates[:, None, None, None]
    master_new = master - layer_rate * direction
    teacher_new = EMA_KEEP * teacher + (1.0 - EMA_KEEP) * master_new
    return (master_new, teacher_new, first_new, second_new, master_new.astype(jnp.bfloat16), teacher_new.astype(jnp.bfloat16))
```

```python
import functools
import math

import jax
import jax.numpy as jnp
from jax import lax
from jax.experimental import pallas as pl
from jax.experimental.pallas import tpu as pltpu
from jax.sharding import PartitionSpec as P

CLIP_NORM = 0.1
BETA_ONE = 0.9
BETA_TWO = 0.999
BIAS_ONE = 1.0 - 0.9**50 * 0.9**50
BIAS_TWO = 1.0 - 0.999**50 * 0.999**50
ADAM_EPS = 1e-08
DECAY = 0.05
EMA_KEEP = 0.95
MESH = pl.DeviceIdType.MESH


def updated(mean_grad, clip_factor, master, teacher, first_moment, second_moment, layer_rate):
    clipped = clip_factor * mean_grad
    first_new = BETA_ONE * first_moment + (1.0 - BETA_ONE) * clipped
    second_new = BETA_TWO * second_moment + (1.0 - BETA_TWO) * clipped * clipped
    direction = first_new / BIAS_ONE / (jnp.sqrt(second_new / BIAS_TWO) + ADAM_EPS) + DECAY * master
    master_new = master - layer_rate * direction
    teacher_new = EMA_KEEP * teacher + (1.0 - EMA_KEEP) * master_new
    return master_new, teacher_new, first_new, second_new


def plain_shards(gradients, master, teacher, first_moment, second_moment, layer_rates):
    own_grad = gradients[0].astype(jnp.float32)
    summed = lax.psum_scatter(own_grad, ("dp", "fsdp"), scatter_dimension=2, tiled=True)
    mean_grad = summed / (lax.axis_size("dp") * lax.axis_size("fsdp"))
    norm_sq = lax.psum(jnp.sum(mean_grad * mean_grad), ("dp", "fsdp", "mp"))
    clip_factor = jnp.minimum(1.0, CLIP_NORM / (jnp.sqrt(norm_sq) + 1e-06))
    layer_rate = layer_rates[:, None, None, None]
    new = updated(mean_grad, clip_factor, master, teacher, first_moment, second_moment, layer_rate)
    student_half, teacher_half = new[0].astype(jnp.bfloat16), new[1].astype(jnp.bfloat16)
    return (
        *new,
        lax.all_gather(student_half, ("dp", "fsdp"), axis=2, tiled=True),
        lax.all_gather(teacher_half, ("dp", "fsdp"), axis=2, tiled=True),
    )


def step_kernel(
    sizes, chunks, grad, master, teacher, first, second, rates,
    master_out, teacher_out, first_out, second_out, student_w, teacher_w,
    own, met, mean, state, fresh, half, norm_own, norm_met,
    own_sem, state_sem, out_sem, half_sem,
    a_send, a_recv, n_send, n_recv, g_send, g_recv, f_send, f_recv,
):
    nd, nf, nm = sizes
    x, z, m = lax.axis_index("dp"), lax.axis_index("fsdp"), lax.axis_index("mp")
    slabs, rows, width = mean.shape
    per = slabs // chunks
    halves = slabs // rates.shape[0]
    total = nd * nf
    place = pl.ds(pl.multiple_of((x * nf + z) * rows, rows), rows)
    cut = [pl.ds(k * per, per) for k in range(chunks)]
    peers = [(a, b) for a in range(nd) for b in range(nf) if (a, b) != (0, 0)]

    def at_x(a):
        return lax.rem(x + a, nd)

    def at_z(b):
        return lax.rem(z + b, nf)

    def at_m(c):
        return lax.rem(m + c, nm)

    def remote(src, dst, send, recv, **where):
        return pltpu.make_async_remote_copy(
            src_ref=src, dst_ref=dst, send_sem=send, recv_sem=recv, device_id=where, device_id_type=MESH
        )

    barrier = pltpu.get_barrier_semaphore()
    for a, b in peers:
        pl.semaphore_signal(barrier, inc=1, device_id={"dp": at_x(a), "fsdp": at_z(b)}, device_id_type=MESH)
    for c in range(1, nm):
        pl.semaphore_signal(barrier, inc=1, device_id={"mp": at_m(c)}, device_id_type=MESH)

    takes = [pltpu.make_async_copy(grad.at[cut[k], place, :], own.at[cut[k]], own_sem.at[k]) for k in range(chunks)]
    for take in takes:
        take.start()
    loads = [pltpu.make_async_copy(ref, state.at[i], state_sem.at[i]) for i, ref in enumerate((master, teacher, first, second))]
    pl.semaphore_wait(barrier, len(peers) + nm - 1)

    sent = {}
    for k in range(chunks):
        for i, (a, b) in enumerate(peers):
            theirs = pl.ds(pl.multiple_of((at_x(a) * nf + at_z(b)) * rows, rows), rows)
            sent[k, i] = remote(
                grad.at[cut[k], theirs, :], met.at[i, cut[k]], a_send.at[i, k], a_recv.at[i, k], dp=at_x(a), fsdp=at_z(b)
            )
            sent[k, i].start()
    for load in loads:
        load.start()

    square = jnp.zeros((8, 128), jnp.float32)
    for k in range(chunks):
        takes[k].wait()
        for i in range(len(peers)):
            sent[k, i].wait_recv()
        for s in range(k * per, (k + 1) * per):
            value = own[s].astype(jnp.float32)
            for i in range(len(peers)):
                value = value + met[i, s].astype(jnp.float32)
            value = value / total
            mean[s] = value
            for part in range(width // 128):
                lane = value[:, part * 128:(part + 1) * 128]
                square = square + jnp.sum((lane * lane).reshape(-1, 8, 128), axis=0)

    norm_own[0] = square
    told = []
    for i, (a, b) in enumerate(peers):
        told.append(remote(norm_own.at[0], norm_met.at[i], n_send.at[i], n_recv.at[i], dp=at_x(a), fsdp=at_z(b)))
        told[-1].start()
    for load in loads:
        load.wait()
    for i in range(len(peers)):
        told[i].wait_recv()
        square = square + norm_met[i]
    norm_own[1] = square
    for c in range(1, nm):
        i = len(peers) + c - 1
        told.append(remote(norm_own.at[1], norm_met.at[i], n_send.at[i], n_recv.at[i], mp=at_m(c)))
        told[-1].start()
    for c in range(1, nm):
        i = len(peers) + c - 1
        told[i].wait_recv()
        square = square + norm_met[i]
    norm_sq = jnp.sum(jnp.sum(square, axis=0, keepdims=True), axis=1, keepdims=True)
    clip_factor = jnp.minimum(1.0, CLIP_NORM / (jnp.sqrt(norm_sq) + 1e-06))

    weights = (student_w, teacher_w)
    spread, stores = [], []
    gathered = {}
    for k in range(chunks):
        for s in range(k * per, (k + 1) * per):
            new = updated(
                mean[s], clip_factor, state[0, s], state[1, s], state[2, s], state[3, s], rates[s // halves]
            )
            for i in range(4):
                fresh[i, s] = new[i]
            for w in range(2):
                half[w, s] = new[w].astype(jnp.bfloat16)
        for w in range(2):
            for b in range(1, nf):
                gathered[k, b, w] = remote(
                    half.at[w, cut[k]], weights[w].at[cut[k], place, :],
                    g_send.at[w, b - 1, k], g_recv.at[w, b - 1, k], fsdp=at_z(b),
                )
                gathered[k, b, w].start()
            for a in range(1, nd):
                spread.append(remote(
                    half.at[w, cut[k]], weights[w].at[cut[k], place, :],
                    f_send.at[w, 0, a - 1, k], f_recv.at[w, 0, a - 1, k], dp=at_x(a),
                ))
                spread[-1].start()
            stores.append(pltpu.make_async_copy(half.at[w, cut[k]], weights[w].at[cut[k], place, :], half_sem.at[w, k]))
            stores[-1].start()
    for i, ref in enumerate((master_out, teacher_out, first_out, second_out)):
        stores.append(pltpu.make_async_copy(fresh.at[i], ref, out_sem.at[i]))
        stores[-1].start()

    for k in range(chunks):
        for b in range(1, nf):
            source = pl.ds(pl.multiple_of((x * nf + lax.rem(z + nf - b, nf)) * rows, rows), rows)
            for w in range(2):
                gathered[k, b, w].wait_recv()
                for a in range(1, nd):
                    there = weights[w].at[cut[k], source, :]
                    spread.append(remote(
                        there, there, f_send.at[w, b, a - 1, k], f_recv.at[w, b, a - 1, k], dp=at_x(a)
                    ))
                    spread[-1].start()
    for copy in stores:
        copy.wait()
    for copy in (*sent.values(), *told, *gathered.values()):
        copy.wait_send()
    for copy in spread:
        copy.wait()


def kernel_shards(sizes, gradients, master, teacher, first_moment, second_moment, layer_rates):
    nd, nf, nm = sizes
    layers, two, rows, width = master.shape
    slabs, full = layers * two, gradients.shape[3]
    chunks = math.gcd(layers, 6)
    shard = (slabs, rows, width)
    f32 = jnp.float32
    anywhere = pl.BlockSpec(memory_space=pl.ANY)
    dma = pltpu.SemaphoreType.DMA
    peers = nd * nf - 1 + nm - 1
    outs = pl.pallas_call(
        functools.partial(step_kernel, sizes, chunks),
        out_shape=[jax.ShapeDtypeStruct(shard, f32)] * 4 + [jax.ShapeDtypeStruct((slabs, full, width), jnp.bfloat16)] * 2,
        in_specs=[anywhere] * 5 + [pl.BlockSpec(memory_space=pltpu.SMEM)],
        out_specs=[anywhere] * 6,
        scratch_shapes=[
            pltpu.VMEM(shard, jnp.bfloat16),
            pltpu.VMEM((nd * nf - 1, *shard), jnp.bfloat16),
            pltpu.VMEM(shard, f32),
            pltpu.VMEM((4, *shard), f32),
            pltpu.VMEM((4, *shard), f32),
            pltpu.VMEM((2, *shard), jnp.bfloat16),
            pltpu.VMEM((2, 8, 128), f32),
            pltpu.VMEM((peers, 8, 128), f32),
            dma((chunks,)), dma((4,)), dma((4,)), dma((2, chunks)),
            dma((nd * nf - 1, chunks)), dma((nd * nf - 1, chunks)),
            dma((peers,)), dma((peers,)),
            dma((2, nf - 1, chunks)), dma((2, nf - 1, chunks)),
            dma((2, nf, nd - 1, chunks)), dma((2, nf, nd - 1, chunks)),
        ],
        compiler_params=pltpu.CompilerParams(
            collective_id=0, has_side_effects=True, vmem_limit_bytes=40 * 1024 * 1024
        ),
    )(
        gradients.reshape(slabs, full, width),
        *(held.reshape(shard) for held in (master, teacher, first_moment, second_moment)),
        layer_rates,
    )
    return tuple(out.reshape(layers, two, *out.shape[1:]) for out in outs)


def shards(sizes, gradients, *rest):
    nd, nf, _ = sizes
    rows, width = rest[0].shape[2:]
    if nd > 1 and nf > 1 and rows % 32 == 0 and width % 128 == 0:
        return kernel_shards(sizes, gradients, *rest)
    return plain_shards(gradients, *rest)


def solution(mesh):
    held = P(None, None, ("dp", "fsdp"), "mp")
    whole = P(None, None, None, "mp")
    sizes = tuple(mesh.shape[axis] for axis in ("dp", "fsdp", "mp"))
    return jax.shard_map(
        functools.partial(shards, sizes),
        mesh=mesh,
        in_specs=(P(("dp", "fsdp"), None, None, None, "mp"), held, held, held, held, P()),
        out_specs=(held, held, held, held, whole, whole),
        check_vma=False,
    )
```

```python
import functools
import math

import jax
import jax.numpy as jnp
from jax import lax
from jax.experimental import pallas as pl
from jax.experimental.pallas import tpu as pltpu
from jax.sharding import PartitionSpec as P

CLIP_NORM = 0.1
BETA_ONE = 0.9
BETA_TWO = 0.999
BIAS_ONE = 1.0 - 0.9**50 * 0.9**50
BIAS_TWO = 1.0 - 0.999**50 * 0.999**50
ADAM_EPS = 1e-08
DECAY = 0.05
EMA_KEEP = 0.95
MESH = pl.DeviceIdType.MESH


def updated(mean_grad, clip_factor, master, teacher, first_moment, second_moment, layer_rate):
    clipped = clip_factor * mean_grad
    first_new = BETA_ONE * first_moment + (1.0 - BETA_ONE) * clipped
    second_new = BETA_TWO * second_moment + (1.0 - BETA_TWO) * clipped * clipped
    direction = first_new / BIAS_ONE / (jnp.sqrt(second_new / BIAS_TWO) + ADAM_EPS) + DECAY * master
    master_new = master - layer_rate * direction
    teacher_new = EMA_KEEP * teacher + (1.0 - EMA_KEEP) * master_new
    return master_new, teacher_new, first_new, second_new


def plain_shards(gradients, master, teacher, first_moment, second_moment, layer_rates):
    own_grad = gradients[0].astype(jnp.float32)
    summed = lax.psum_scatter(own_grad, ("dp", "fsdp"), scatter_dimension=2, tiled=True)
    mean_grad = summed / (lax.axis_size("dp") * lax.axis_size("fsdp"))
    norm_sq = lax.psum(jnp.sum(mean_grad * mean_grad), ("dp", "fsdp", "mp"))
    clip_factor = jnp.minimum(1.0, CLIP_NORM / (jnp.sqrt(norm_sq) + 1e-06))
    layer_rate = layer_rates[:, None, None, None]
    new = updated(mean_grad, clip_factor, master, teacher, first_moment, second_moment, layer_rate)
    student_half, teacher_half = new[0].astype(jnp.bfloat16), new[1].astype(jnp.bfloat16)
    return (
        *new,
        lax.all_gather(student_half, ("dp", "fsdp"), axis=2, tiled=True),
        lax.all_gather(teacher_half, ("dp", "fsdp"), axis=2, tiled=True),
    )


def step_kernel(
    sizes, chunks, grad, master, teacher, first, second, rates,
    master_out, teacher_out, first_out, second_out, student_w, teacher_w,
    own, met, mean, norm_own, norm_met,
    own_sem,
    a_send, a_recv, n_send, n_recv, g_send, g_recv, e_send, e_recv, f_send, f_recv,
):
    nd, nf, nm = sizes
    x, z, m = lax.axis_index("dp"), lax.axis_index("fsdp"), lax.axis_index("mp")
    slabs, rows, width = mean.shape
    per = slabs // chunks
    halves = slabs // rates.shape[0]
    total = nd * nf
    place = pl.ds(pl.multiple_of((x * nf + z) * rows, rows), rows)
    cut = [pl.ds(k * per, per) for k in range(chunks)]
    peers = [(a, b) for a in range(nd) for b in range(nf) if (a, b) != (0, 0)]

    def at_x(a):
        return lax.rem(x + a, nd)

    def at_z(b):
        return lax.rem(z + b, nf)

    def at_m(c):
        return lax.rem(m + c, nm)

    def remote(src, dst, send, recv, **where):
        return pltpu.make_async_remote_copy(
            src_ref=src, dst_ref=dst, send_sem=send, recv_sem=recv, device_id=where, device_id_type=MESH
        )

    barrier = pltpu.get_barrier_semaphore()
    for a, b in peers:
        pl.semaphore_signal(barrier, inc=1, device_id={"dp": at_x(a), "fsdp": at_z(b)}, device_id_type=MESH)
    for c in range(1, nm):
        pl.semaphore_signal(barrier, inc=1, device_id={"mp": at_m(c)}, device_id_type=MESH)

    takes = [pltpu.make_async_copy(grad.at[cut[k], place, :], own.at[cut[k]], own_sem.at[k]) for k in range(chunks)]
    for take in takes:
        take.start()
    pl.semaphore_wait(barrier, len(peers) + nm - 1)

    sent = {}
    for k in range(chunks):
        for i, (a, b) in enumerate(peers):
            theirs = pl.ds(pl.multiple_of((at_x(a) * nf + at_z(b)) * rows, rows), rows)
            sent[k, i] = remote(
                grad.at[cut[k], theirs, :], met.at[i, cut[k]], a_send.at[i, k], a_recv.at[i, k], dp=at_x(a), fsdp=at_z(b)
            )
            sent[k, i].start()

    square = jnp.zeros((8, 128), jnp.float32)
    for k in range(chunks):
        takes[k].wait()
        for i in range(len(peers)):
            sent[k, i].wait_recv()
        for s in range(k * per, (k + 1) * per):
            value = own[s].astype(jnp.float32)
            for i in range(len(peers)):
                value = value + met[i, s].astype(jnp.float32)
            value = value / total
            mean[s] = value
            for part in range(width // 128):
                lane = value[:, part * 128:(part + 1) * 128]
                square = square + jnp.sum((lane * lane).reshape(-1, 8, 128), axis=0)

    norm_own[0] = square
    told = []
    for i, (a, b) in enumerate(peers):
        told.append(remote(norm_own.at[0], norm_met.at[i], n_send.at[i], n_recv.at[i], dp=at_x(a), fsdp=at_z(b)))
        told[-1].start()
    for i in range(len(peers)):
        told[i].wait_recv()
        square = square + norm_met[i]
    norm_own[1] = square
    for c in range(1, nm):
        i = len(peers) + c - 1
        told.append(remote(norm_own.at[1], norm_met.at[i], n_send.at[i], n_recv.at[i], mp=at_m(c)))
        told[-1].start()
    for c in range(1, nm):
        i = len(peers) + c - 1
        told[i].wait_recv()
        square = square + norm_met[i]
    norm_sq = jnp.sum(jnp.sum(square, axis=0, keepdims=True), axis=1, keepdims=True)
    clip_factor = jnp.minimum(1.0, CLIP_NORM / (jnp.sqrt(norm_sq) + 1e-06))

    weights = (student_w, teacher_w)
    news = (master_out, teacher_out, first_out, second_out)
    last = nf - 1

    def bands(k, column, row):
        return [ref.at[cut[k], pl.ds(pl.multiple_of((column * nf + row) * rows, rows), rows), :] for ref in weights]

    def along(way, k, d):
        there = bands(k, x, z - d if way == 0 else z + d)
        return [
            remote(there[w], there[w], g_send.at[way, w, d, k], g_recv.at[way, w, d, k], fsdp=z + 1 if way == 0 else z - 1)
            for w in range(2)
        ]

    def arriving(way, k, d):
        there = bands(k, x, z - d if way == 0 else z + d)
        return [remote(there[w], there[w], g_send.at[way, w, d, k], g_recv.at[way, w, d - 1, k], fsdp=z) for w in range(2)]

    def far(way, k):
        there = bands(k, 1 - x, 0 if way == 0 else last)
        return [
            remote(there[w], there[w], e_send.at[way, w, k], e_recv.at[way, w, k], fsdp=z + 1 if way == 0 else z - 1)
            for w in range(2)
        ]

    def across(way, k, d):
        there = bands(k, x, z - d if way == 0 else z + d)
        return [
            remote(there[w], there[w], f_send.at[way, w, d, k], f_recv.at[way, w, d, k], dp=1 - x) for w in range(2)
        ]

    def start(copies):
        for copy in copies:
            copy.start()

    def wait_recv(copies):
        for copy in copies:
            copy.wait_recv()

    def wait_send(copies):
        for copy in copies:
            copy.wait_send()

    inner = (z < last, z > 0)
    origin = (z == 0, z == last)

    def has(way, d):
        return z >= d if way == 0 else z + d <= last

    def crosses(way, k, d):
        from_end = z == d if way == 0 else z + d == last
        return jnp.logical_and(has(way, d), jnp.logical_not(from_end)) if k % 2 else has(way, d)

    for k in range(chunks):
        for s in range(k * per, (k + 1) * per):
            new = updated(
                mean[s], clip_factor, master[s], teacher[s], first[s], second[s], rates[s // halves]
            )
            for i in range(4):
                news[i][s] = new[i]
            for w in range(2):
                weights[w][s, place, :] = new[w].astype(jnp.bfloat16)
        start(across(0, k, 0))
        for way in range(2):
            pl.when(inner[way])(lambda way=way: start(along(way, k, 0)))

    odd = range(1, chunks, 2)
    for k in odd:
        wait_recv(across(0, k, 0))
        for way in range(2):
            pl.when(origin[way])(lambda way=way, k=k: start(far(way, k)))
    for d in range(1, nf):
        for k in range(chunks):
            for way in range(2):
                @pl.when(has(way, d))
                def _(way=way, d=d, k=k):
                    wait_recv(arriving(way, k, d))
                    pl.when(inner[way])(lambda: start(along(way, k, d)))
                    pl.when(crosses(way, k, d))(lambda: start(across(way, k, d)))
        for k in odd:
            for way in range(2):
                @pl.when(z == d if way == 0 else z == last - d)
                def _(way=way, k=k):
                    wait_recv(far(way, k))
                    pl.when(inner[way])(lambda: start(far(way, k)))

    for copy in (*sent.values(), *told):
        copy.wait_send()
    for k in range(chunks):
        if k % 2 == 0:
            wait_recv(across(0, k, 0))
        wait_send(across(0, k, 0))
        for way in range(2):
            for d in range(nf):
                @pl.when(jnp.logical_and(has(way, d), inner[way]))
                def _(way=way, d=d, k=k):
                    wait_send(along(way, k, d))
                if d:
                    @pl.when(crosses(way, k, d))
                    def _(way=way, d=d, k=k):
                        wait_recv(across(way, k, d))
                        wait_send(across(way, k, d))
            if k % 2:
                pl.when(inner[way])(lambda way=way, k=k: wait_send(far(way, k)))


def kernel_shards(sizes, gradients, master, teacher, first_moment, second_moment, layer_rates):
    nd, nf, nm = sizes
    layers, two, rows, width = master.shape
    slabs, full = layers * two, gradients.shape[3]
    chunks = math.gcd(layers, 6)
    shard = (slabs, rows, width)
    f32 = jnp.float32
    outside = pl.BlockSpec(memory_space=pltpu.HBM)
    inside = pl.BlockSpec(memory_space=pltpu.VMEM)
    dma = pltpu.SemaphoreType.DMA
    peers = nd * nf - 1 + nm - 1
    outs = pl.pallas_call(
        functools.partial(step_kernel, sizes, chunks),
        out_shape=[jax.ShapeDtypeStruct(shard, f32)] * 4 + [jax.ShapeDtypeStruct((slabs, full, width), jnp.bfloat16)] * 2,
        in_specs=[outside] + [inside] * 4 + [pl.BlockSpec(memory_space=pltpu.SMEM)],
        out_specs=[inside] * 6,
        scratch_shapes=[
            pltpu.VMEM(shard, jnp.bfloat16),
            pltpu.VMEM((nd * nf - 1, *shard), jnp.bfloat16),
            pltpu.VMEM(shard, f32),
            pltpu.VMEM((2, 8, 128), f32),
            pltpu.VMEM((peers, 8, 128), f32),
            dma((chunks,)),
            dma((nd * nf - 1, chunks)), dma((nd * nf - 1, chunks)),
            dma((peers,)), dma((peers,)),
            dma((2, 2, nf, chunks)), dma((2, 2, nf, chunks)),
            dma((2, 2, chunks)), dma((2, 2, chunks)),
            dma((2, 2, nf, chunks)), dma((2, 2, nf, chunks)),
        ],
        compiler_params=pltpu.CompilerParams(
            collective_id=0, has_side_effects=True, vmem_limit_bytes=40 * 1024 * 1024
        ),
    )(
        gradients.reshape(slabs, full, width),
        *(held.reshape(shard) for held in (master, teacher, first_moment, second_moment)),
        layer_rates,
    )
    return tuple(out.reshape(layers, two, *out.shape[1:]) for out in outs)


def shards(sizes, gradients, *rest):
    nd, nf, _ = sizes
    rows, width = rest[0].shape[2:]
    if nd == 2 and nf > 1 and rows % 32 == 0 and width % 128 == 0:
        return kernel_shards(sizes, gradients, *rest)
    return plain_shards(gradients, *rest)


def solution(mesh):
    held = P(None, None, ("dp", "fsdp"), "mp")
    whole = P(None, None, None, "mp")
    sizes = tuple(mesh.shape[axis] for axis in ("dp", "fsdp", "mp"))
    return jax.shard_map(
        functools.partial(shards, sizes),
        mesh=mesh,
        in_specs=(P(("dp", "fsdp"), None, None, None, "mp"), held, held, held, held, P()),
        out_specs=(held, held, held, held, whole, whole),
        check_vma=False,
    )
```
